32 devices in a mesh: bank: 4 (over y, x), zero: 8 (over z, core).
Axes of the slice: x: 2, y: 2, z: 4, core: 2. Of those that a mesh axis runs over, the one named last changes fastest.
Arguments:
- master_gate: float32 [64, 2048, 1024], P('bank', 'zero'), may hold values from -0.1875 to 0.1875
- master_up: float32 [64, 2048, 1024], P('bank', 'zero'), may hold values from -0.1875 to 0.1875
- master_down: float32 [64, 1024, 2048], P('bank', None, 'zero'), may hold values from -0.25 to 0.25
- router_weight: float32 [2048, 64], P('zero', 'bank'), may hold values from -0.125 to 0.125
- router_gain: float32 [2048], P('zero'), may hold values from 0.25 to 1.75
Outputs:
- final_gate: bfloat16 [64, 2048, 1024], P('bank', None, 'zero')
- final_up: bfloat16 [64, 2048, 1024], P('bank', None, 'zero')
- final_down: bfloat16 [64, 1024, 2048], P('bank', 'zero')
- scale_gate: float32 [64, 1024], P('bank', 'zero')
- scale_up: float32 [64, 1024], P('bank', 'zero')
- scale_down: float32 [64, 1024], P('bank', 'zero')
- serve_router: bfloat16 [2048, 64], replicated
The draws below stay inside these ranges and needn't reach their ends.
All inputs are finite; a program needn't handle non-finite values.
Results may differ from the reference program's by a relative error of at most 0.0085.
Values may be sent and summed in bfloat16 or wider, within the bound.
A program may use at most 192 MiB of HBM per device.

```python
import jax
import jax.numpy as jnp
from jax import lax

EXPERTS = 64
D_MODEL = 2048
D_EXPERT = 1024


def raised(values, own_key, source, target, shards_of, factor):
    owner, partner = [(jnp.arange(values.shape[position]) // (values.shape[position] // shards_of)).reshape([-1 if axis == position else 1 for axis in range(values.ndim)]) for position in (source, target)]
    chosen = jax.random.permutation(own_key, shards_of)[partner]
    strong = (owner == chosen) | (owner == (partner + shards_of // 2) % shards_of)
    return jnp.where(strong, factor * values, values)


def block_levels(own_key, shape, pieces, low, largest):
    gain, own = 1.0, jax.random.fold_in(own_key, 6)
    for axis_at, parts in pieces:
        draws = jnp.exp(jax.random.uniform(jax.random.fold_in(own, axis_at), (parts,), jnp.float32, low / len(pieces), largest / len(pieces)))
        gain = gain * jnp.repeat(draws, shape[axis_at] // parts).reshape([-1 if axis == axis_at else 1 for axis in range(len(shape))])
    return gain


def centred(stream_key, shape, width, limit, split=(), dtype=jnp.bfloat16):
    array = jax.random.normal(stream_key, shape, jnp.float32) * width
    if len(split) > 0:
        array = block_levels(stream_key, shape, split, -0.22, 0.18) * array
    return jnp.clip(array, min=-limit, max=limit).astype(dtype)


def gaussian_with(rng, extent, width, reach, pieces, heavy, held_as=jnp.bfloat16):
    drawn = width * jax.random.normal(rng, extent, jnp.float32)
    if pieces:
        drawn = drawn * block_levels(rng, extent, pieces, -0.22, 0.18)
    return jnp.clip(raised(drawn, jax.random.fold_in(rng, 3), *heavy), -reach, reach).astype(held_as)


def setup_inputs(seed: int = 0) -> dict:
    seeds = jax.random.split(jax.random.key(seed), 6)
    master_gate = gaussian_with(seeds[0], (EXPERTS, D_MODEL, D_EXPERT), D_MODEL ** -0.5, 0.1875, ((0, 4), (1, 8)), (1, 2, 8, 2.0), jnp.float32)
    master_up = gaussian_with(seeds[1], (EXPERTS, D_MODEL, D_EXPERT), D_MODEL ** -0.5, 0.1875, ((0, 4), (1, 8)), (1, 2, 8, 2.0), jnp.float32)
    master_down = gaussian_with(seeds[2], (EXPERTS, D_EXPERT, D_MODEL), D_EXPERT ** -0.5, 0.25, ((0, 4), (2, 8)), (2, 1, 8, 2.0), jnp.float32)
    router_weight = centred(seeds[3], (D_MODEL, EXPERTS), D_MODEL ** -0.5, 0.125, ((0, 8), (1, 4)), jnp.float32)
    router_gain = jnp.clip(1.0 + 0.15 * jax.random.normal(seeds[4], (D_MODEL,), jnp.float32), 0.25, 1.75)
    return dict(master_gate=master_gate, master_up=master_up, master_down=master_down, router_weight=router_weight, router_gain=router_gain)


def reference(master_gate, master_up, master_down, router_weight, router_gain):
    scale_gate = jnp.sqrt(lax.optimization_barrier(jnp.sum(master_gate * master_gate, axis=1)))
    final_gate = (master_gate / jnp.expand_dims(scale_gate, 1)).astype(jnp.bfloat16)
    scale_up = jnp.sqrt(lax.optimization_barrier(jnp.sum(master_up * master_up, axis=1)))
    final_up = (master_up / jnp.expand_dims(scale_up, 1)).astype(jnp.bfloat16)
    scale_down = jnp.sqrt(lax.optimization_barrier(jnp.sum(master_down * master_down, axis=2)))
    final_down = (master_down / jnp.expand_dims(scale_down, 2)).astype(jnp.bfloat16)
    serve_router = (router_weight * router_gain[:, None]).astype(jnp.bfloat16)
    return (final_gate, final_up, final_down, scale_gate, scale_up, scale_down, serve_router)
```

```python
import functools

import jax
import jax.numpy as jnp
from jax import lax
from jax.experimental import pallas as pl
from jax.experimental.pallas import tpu as pltpu
from jax.sharding import PartitionSpec as P

MESH = pl.DeviceIdType.MESH
LANES = 128
ROWS = 16
GROUP = 2


def far_first(n):
    return sorted(range(1, n), key=lambda j: (abs(2 * j - n), j))


def exchange_kernel(
    n, banks,
    gate, up, down, weight, gain,
    out_gate, out_up, out_down, out_router,
    stage_gate, stage_up, stage_down, send_gate, send_up, send_down, part, router,
    load_sem, own_sem, send_sem, recv_sem, row_sem, column_sem,
):
    me, bank = lax.axis_index("zero"), lax.axis_index("bank")
    experts = gate.shape[0]
    groups = experts // GROUP
    ins, stages = (gate, up, down), (stage_gate, stage_up, stage_down)
    sends, outs = (send_gate, send_up, send_down), (out_gate, out_up, out_down)
    order = far_first(n)

    def peer(j):
        return lax.rem(me + j, n)

    def bank_peer(j):
        return lax.rem(bank + j, banks)

    def load(a, g):
        slot = lax.rem(g, 2)
        return pltpu.make_async_copy(
            ins[a].at[pl.ds(g * GROUP, GROUP)], stages[a].at[slot], load_sem.at[a, slot]
        )

    def place(a, g):
        chosen = pl.ds(g * GROUP, GROUP)
        if a < 2:
            height = gate.shape[1]
            return outs[a].at[chosen, pl.ds(pl.multiple_of(me * height, height), height), :]
        width = down.shape[2]
        return outs[a].at[chosen, :, pl.ds(pl.multiple_of(me * width, width), width)]

    def remote(a, g, j):
        return pltpu.make_async_remote_copy(
            src_ref=sends[a].at[peer(j), pl.ds(g * GROUP, GROUP)],
            dst_ref=place(a, g),
            send_sem=send_sem.at[a, g, j],
            recv_sem=recv_sem.at[a, g, j],
            device_id={"zero": peer(j)},
            device_id_type=MESH,
        )

    def own(a, g):
        return pltpu.make_async_copy(
            sends[a].at[me, pl.ds(g * GROUP, GROUP)], place(a, g), own_sem.at[a, g]
        )

    def narrow(a, g):
        slot = lax.rem(g, 2)
        load(a, g).wait()
        for d in range(n):
            if a < 2:
                wide = send_gate.shape[3]
                piece = stages[a][slot, :, :, d * wide : (d + 1) * wide]
            else:
                tall = send_down.shape[2]
                piece = stages[a][slot, :, d * tall : (d + 1) * tall, :]
            sends[a][d, pl.ds(g * GROUP, GROUP)] = piece.astype(jnp.bfloat16)

        @pl.when(g + 2 < groups)
        def _():
            load(a, g + 2).start()

    def send(a, g):
        for j in order:
            remote(a, g, j).start()
        own(a, g).start()

    rows, columns = weight.shape
    my_rows = pl.ds(pl.multiple_of(bank * rows, rows), rows)
    my_columns = pl.ds(pl.multiple_of(me * columns, columns), columns)

    def send_rows(j):
        return pltpu.make_async_remote_copy(
            src_ref=part,
            dst_ref=router.at[my_rows, my_columns],
            send_sem=row_sem.at[0, j],
            recv_sem=row_sem.at[1, j],
            device_id={"zero": peer(j)},
            device_id_type=MESH,
        )

    def send_columns(j):
        return pltpu.make_async_remote_copy(
            src_ref=router.at[my_rows],
            dst_ref=router.at[my_rows],
            send_sem=column_sem.at[0, j],
            recv_sem=column_sem.at[1, j],
            device_id={"bank": bank_peer(j)},
            device_id_type=MESH,
        )

    for a in range(3):
        for g in range(min(2, groups)):
            load(a, g).start()
    barrier = pltpu.get_barrier_semaphore()
    for j in range(1, n):
        pl.semaphore_signal(barrier, inc=1, device_id={"zero": peer(j)}, device_id_type=MESH)
    for j in range(1, banks):
        pl.semaphore_signal(barrier, inc=1, device_id={"bank": bank_peer(j)}, device_id_type=MESH)
    folded = (weight[...] * gain[...]).astype(jnp.bfloat16)
    part[...] = folded
    router[my_rows, my_columns] = folded
    narrow(0, 0)
    pl.semaphore_wait(barrier, n - 1 + banks - 1)

    for j in order:
        send_rows(j).start()

    def step(g, carry):
        @pl.when(g > 0)
        def _():
            narrow(0, g)
            send(2, g - 1)

        narrow(1, g)
        send(0, g)
        narrow(2, g)
        send(1, g)
        return carry

    lax.fori_loop(0, groups, step, 0)
    for j in order:
        send_rows(j).wait()
    send(2, groups - 1)
    for j in range(1, banks):
        send_columns(j).start()
    for j in range(1, banks):
        send_columns(j).wait()
    out_router[...] = router[...]

    def finish(g, carry):
        for a in range(3):
            own(a, g).wait()
            for j in order:
                remote(a, g, j).wait()
        return carry

    lax.fori_loop(0, groups, finish, 0)


def scale_kernel(gate, up, down, out_gate, out_up, out_down, scale_gate, scale_up, scale_down):
    e = pl.program_id(0)
    for source, target, scales in ((gate, out_gate, scale_gate), (up, out_up, scale_up)):
        values = source[0].astype(jnp.float32)
        scale = jnp.sqrt(jnp.sum(values * values, axis=0, keepdims=True))
        scales[pl.ds(e, 1), :] = scale
        target[0] = (values * (1.0 / scale)).astype(jnp.bfloat16)
    values = down[0].astype(jnp.float32)
    scale = jnp.sqrt(jnp.sum(values * values, axis=1, keepdims=True))
    tall = scale.shape[0]
    scale_down[pl.ds(e, 1), :] = jnp.broadcast_to(scale, (tall, LANES)).T[0:1, :]
    out_down[0] = (values * (1.0 / scale)).astype(jnp.bfloat16)


def fused(n, banks, master_gate, master_up, master_down, router_weight, router_gain):
    experts, height, width = master_gate.shape
    inner, share = master_down.shape[1:]
    columns, rows = router_weight.shape
    narrow = jnp.bfloat16
    any_space = pl.BlockSpec(memory_space=pl.ANY)
    vmem = pl.BlockSpec(memory_space=pltpu.VMEM)
    groups = experts // GROUP
    shape_gate = jax.ShapeDtypeStruct((experts, height * n, width // n), narrow)
    shape_down = jax.ShapeDtypeStruct((experts, inner // n, share * n), narrow)
    piece = 2 * experts * (2 * height * width + inner * share)
    raw_gate, raw_up, raw_down, router = pl.pallas_call(
        functools.partial(exchange_kernel, n, banks),
        out_shape=(
            shape_gate,
            shape_gate,
            shape_down,
            jax.ShapeDtypeStruct((rows * banks, columns * n), narrow),
        ),
        in_specs=[any_space] * 3 + [vmem] * 2,
        out_specs=[any_space] * 3 + [vmem],
        scratch_shapes=[
            pltpu.VMEM((2, GROUP, height, width), jnp.float32),
            pltpu.VMEM((2, GROUP, height, width), jnp.float32),
            pltpu.VMEM((2, GROUP, inner, share), jnp.float32),
            pltpu.VMEM((n, experts, height, width // n), narrow),
            pltpu.VMEM((n, experts, height, width // n), narrow),
            pltpu.VMEM((n, experts, inner // n, share), narrow),
            pltpu.VMEM((rows, columns), narrow),
            pltpu.VMEM((rows * banks, columns * n), narrow),
            pltpu.SemaphoreType.DMA((3, 2)),
            pltpu.SemaphoreType.DMA((3, groups)),
            pltpu.SemaphoreType.DMA((3, groups, n)),
            pltpu.SemaphoreType.DMA((3, groups, n)),
            pltpu.SemaphoreType.DMA((2, n)),
            pltpu.SemaphoreType.DMA((2, banks)),
        ],
        compiler_params=pltpu.CompilerParams(
            collective_id=0, has_side_effects=True, vmem_limit_bytes=60 * 2**20
        ),
        cost_estimate=pl.CostEstimate(flops=piece, bytes_accessed=3 * piece, transcendentals=0),
        name="exchange",
    )(master_gate, master_up, master_down, router_weight.T, router_gain[None, :])

    def block(shape):
        return pl.BlockSpec((1,) + shape.shape[1:], lambda e: (e, 0, 0))

    def whole(shape):
        return pl.BlockSpec(shape.shape, lambda e: (0, 0))

    scales_gate = jax.ShapeDtypeStruct((experts, width // n), jnp.float32)
    scales_down = jax.ShapeDtypeStruct((experts, inner // n), jnp.float32)
    outs = (shape_gate, shape_gate, shape_down)
    scales = (scales_gate, scales_gate, scales_down)
    results = pl.pallas_call(
        scale_kernel,
        grid=(experts,),
        out_shape=outs + scales,
        in_specs=[block(s) for s in outs],
        out_specs=[block(s) for s in outs] + [whole(s) for s in scales],
        compiler_params=pltpu.CompilerParams(vmem_limit_bytes=60 * 2**20),
        name="scale",
    )(raw_gate, raw_up, raw_down)
    return (*results, router.T)


def plain(master_gate, master_up, master_down, router_weight, router_gain):
    total_gate, total_up, total_down = (
        lax.psum(jnp.sum(master_gate * master_gate, axis=1).astype(jnp.bfloat16), "zero").astype(
            jnp.float32
        ),
        lax.psum(jnp.sum(master_up * master_up, axis=1).astype(jnp.bfloat16), "zero").astype(
            jnp.float32
        ),
        lax.psum(jnp.sum(master_down * master_down, axis=2).astype(jnp.bfloat16), "zero").astype(
            jnp.float32
        ),
    )
    scale_gate = jnp.sqrt(total_gate)
    scale_up = jnp.sqrt(total_up)
    scale_down = jnp.sqrt(total_down)
    narrow_gate, narrow_up, narrow_down = (
        (master_gate / jnp.expand_dims(scale_gate, 1)).astype(jnp.bfloat16),
        (master_up / jnp.expand_dims(scale_up, 1)).astype(jnp.bfloat16),
        (master_down / jnp.expand_dims(scale_down, 2)).astype(jnp.bfloat16),
    )
    final_gate, final_up = (
        lax.all_to_all(narrow_gate, "zero", split_axis=2, concat_axis=1, tiled=True),
        lax.all_to_all(narrow_up, "zero", split_axis=2, concat_axis=1, tiled=True),
    )
    final_down = lax.all_to_all(narrow_down, "zero", split_axis=1, concat_axis=2, tiled=True)
    scale_gate = lax.dynamic_slice_in_dim(
        scale_gate, lax.axis_index("zero") * final_gate.shape[2], final_gate.shape[2], axis=1
    )
    scale_up = lax.dynamic_slice_in_dim(
        scale_up, lax.axis_index("zero") * final_up.shape[2], final_up.shape[2], axis=1
    )
    scale_down = lax.dynamic_slice_in_dim(
        scale_down, lax.axis_index("zero") * final_down.shape[1], final_down.shape[1], axis=1
    )
    part_router = (router_weight * router_gain[:, None]).astype(jnp.bfloat16)
    row_router = lax.all_gather(part_router, "zero", axis=0, tiled=True)
    serve_router = lax.all_gather(row_router, "bank", axis=1, tiled=True)
    return (final_gate, final_up, final_down, scale_gate, scale_up, scale_down, serve_router)


def local(n, banks, master_gate, master_up, master_down, router_weight, router_gain):
    experts, height, width = master_gate.shape
    inner, share = master_down.shape[1:]
    columns, rows = router_weight.shape
    tiled = (
        experts % GROUP == 0
        and height % ROWS == 0
        and width // n == LANES
        and inner // n == LANES
        and share % LANES == 0
        and columns % LANES == 0
        and rows % ROWS == 0
    )
    arrays = (master_gate, master_up, master_down, router_weight, router_gain)
    return fused(n, banks, *arrays) if tiled else plain(*arrays)


def solution(mesh):
    in_specs = (
        P("bank", "zero", None),
        P("bank", "zero", None),
        P("bank", None, "zero"),
        P("zero", "bank"),
        P("zero"),
    )
    out_specs = (
        P("bank", None, "zero"),
        P("bank", None, "zero"),
        P("bank", "zero", None),
        P("bank", "zero"),
        P("bank", "zero"),
        P("bank", "zero"),
        P(),
    )
    body = functools.partial(local, mesh.shape["zero"], mesh.shape["bank"])
    return jax.shard_map(body, mesh=mesh, in_specs=in_specs, out_specs=out_specs, check_vma=False)
```

```python
import functools

import jax
import jax.numpy as jnp
from jax import lax
from jax.experimental import pallas as pl
from jax.experimental.pallas import tpu as pltpu
from jax.sharding import PartitionSpec as P

MESH = pl.DeviceIdType.MESH
LANES = 128
ROWS = 16
GROUP = 2
BATCH = 2


def far_first(n):
    return sorted(range(1, n), key=lambda j: (abs(2 * j - n), j))


def exchange_kernel(
    n, banks,
    gate, up, down, weight, gain,
    out_gate, out_up, out_down, out_router,
    stage_gate, stage_up, stage_down, send_gate, send_up, send_down, part, router,
    load_sem, own_sem, send_sem, recv_sem, row_sem, column_sem,
):
    me, bank = lax.axis_index("zero"), lax.axis_index("bank")
    experts = gate.shape[0]
    groups = experts // GROUP
    ins, stages = (gate, up, down), (stage_gate, stage_up, stage_down)
    sends, outs = (send_gate, send_up, send_down), (out_gate, out_up, out_down)
    order = far_first(n)

    def peer(j):
        return lax.rem(me + j, n)

    def bank_peer(j):
        return lax.rem(bank + j, banks)

    def load(a, g):
        slot = lax.rem(g, 2)
        return pltpu.make_async_copy(
            ins[a].at[pl.ds(g * GROUP, GROUP)], stages[a].at[slot], load_sem.at[a, slot]
        )

    def place(a, g):
        chosen = pl.ds(g * GROUP, GROUP)
        if a < 2:
            height = gate.shape[1]
            return outs[a].at[chosen, pl.ds(pl.multiple_of(me * height, height), height), :]
        width = down.shape[2]
        return outs[a].at[chosen, :, pl.ds(pl.multiple_of(me * width, width), width)]

    def remote(a, g, j):
        return pltpu.make_async_remote_copy(
            src_ref=sends[a].at[peer(j), pl.ds(g * GROUP, GROUP)],
            dst_ref=place(a, g),
            send_sem=send_sem.at[a, g, j],
            recv_sem=recv_sem.at[a, g, j],
            device_id={"zero": peer(j)},
            device_id_type=MESH,
        )

    def own(a, g):
        return pltpu.make_async_copy(
            sends[a].at[me, pl.ds(g * GROUP, GROUP)], place(a, g), own_sem.at[a, g]
        )

    def narrow(a, g):
        slot = lax.rem(g, 2)
        load(a, g).wait()
        for d in range(n):
            if a < 2:
                wide = send_gate.shape[3]
                piece = stages[a][slot, :, :, d * wide : (d + 1) * wide]
            else:
                tall = send_down.shape[2]
                piece = stages[a][slot, :, d * tall : (d + 1) * tall, :]
            sends[a][d, pl.ds(g * GROUP, GROUP)] = piece.astype(jnp.bfloat16)

        @pl.when(g + 2 < groups)
        def _():
            load(a, g + 2).start()

    def send(a, g):
        for j in order:
            remote(a, g, j).start()
        own(a, g).start()

    rows, columns = weight.shape
    my_rows = pl.ds(pl.multiple_of(bank * rows, rows), rows)
    my_columns = pl.ds(pl.multiple_of(me * columns, columns), columns)

    def send_rows(j):
        return pltpu.make_async_remote_copy(
            src_ref=part,
            dst_ref=router.at[my_rows, my_columns],
            send_sem=row_sem.at[0, j],
            recv_sem=row_sem.at[1, j],
            device_id={"zero": peer(j)},
            device_id_type=MESH,
        )

    def send_columns(j):
        return pltpu.make_async_remote_copy(
            src_ref=router.at[my_rows],
            dst_ref=router.at[my_rows],
            send_sem=column_sem.at[0, j],
            recv_sem=column_sem.at[1, j],
            device_id={"bank": bank_peer(j)},
            device_id_type=MESH,
        )

    for a in range(3):
        for g in range(min(2, groups)):
            load(a, g).start()
    barrier = pltpu.get_barrier_semaphore()
    for j in range(1, n):
        pl.semaphore_signal(barrier, inc=1, device_id={"zero": peer(j)}, device_id_type=MESH)
    for j in range(1, banks):
        pl.semaphore_signal(barrier, inc=1, device_id={"bank": bank_peer(j)}, device_id_type=MESH)
    folded = (weight[...] * gain[...]).astype(jnp.bfloat16)
    part[...] = folded
    router[my_rows, my_columns] = folded
    narrow(0, 0)
    pl.semaphore_wait(barrier, n - 1 + banks - 1)

    for j in order:
        send_rows(j).start()

    def step(g, carry):
        @pl.when(g > 0)
        def _():
            narrow(0, g)
            send(2, g - 1)

        narrow(1, g)
        send(0, g)
        narrow(2, g)
        send(1, g)
        return carry

    lax.fori_loop(0, groups, step, 0)
    for j in order:
        send_rows(j).wait()
    send(2, groups - 1)
    for j in range(1, banks):
        send_columns(j).start()
    for j in range(1, banks):
        send_columns(j).wait()
    out_router[...] = router[...]

    def finish(g, carry):
        for a in range(3):
            own(a, g).wait()
            for j in order:
                remote(a, g, j).wait()
        return carry

    lax.fori_loop(0, groups, finish, 0)


def scale_kernel(parts, *refs):
    def expert(i, carry):
        scale_expert(parts, i, *refs)
        return carry

    lax.fori_loop(0, BATCH, expert, 0)


def scale_expert(
    parts, i, gate, up, down, out_gate, out_up, out_down, scale_gate, scale_up, scale_down
):
    e = pl.program_id(0) * BATCH + i
    zeros = jnp.zeros((LANES, LANES), jnp.float32)
    tall = gate.shape[1] // parts
    wide = down.shape[2] // parts

    def rows(c):
        return pl.ds(pl.multiple_of(c * tall, tall), tall)

    def lanes(c):
        return pl.ds(pl.multiple_of(c * wide, wide), wide)

    for source, target, scales in ((gate, out_gate, scale_gate), (up, out_up, scale_up)):

        def add_rows(c, total, source=source):
            values = source[i, rows(c), :].astype(jnp.float32)
            return total + jnp.sum((values * values).reshape(-1, LANES, LANES), axis=0)

        total = lax.fori_loop(0, parts, add_rows, zeros)
        scale = jnp.sqrt(jnp.sum(total, axis=0, keepdims=True))
        scales[pl.ds(e, 1), :] = scale
        inverse = 1.0 / scale

        def put_rows(c, carry, source=source, target=target, inverse=inverse):
            values = source[i, rows(c), :].astype(jnp.float32)
            target[i, rows(c), :] = (values * inverse).astype(jnp.bfloat16)
            return carry

        lax.fori_loop(0, parts, put_rows, 0)

    def add_lanes(c, total):
        values = down[i, :, lanes(c)].astype(jnp.float32)
        for k in range(wide // LANES):
            piece = values[:, k * LANES : (k + 1) * LANES]
            total = total + piece * piece
        return total

    total = lax.fori_loop(0, parts, add_lanes, zeros)
    scale = jnp.sqrt(jnp.sum(total, axis=1, keepdims=True))
    scale_down[pl.ds(e, 1), :] = jnp.broadcast_to(scale, (LANES, LANES)).T[0:1, :]
    inverse = 1.0 / scale

    def put_lanes(c, carry):
        values = down[i, :, lanes(c)].astype(jnp.float32)
        out_down[i, :, lanes(c)] = (values * inverse).astype(jnp.bfloat16)
        return carry

    lax.fori_loop(0, parts, put_lanes, 0)


def fused(n, banks, master_gate, master_up, master_down, router_weight, router_gain):
    experts, height, width = master_gate.shape
    inner, share = master_down.shape[1:]
    columns, rows = router_weight.shape
    narrow = jnp.bfloat16
    any_space = pl.BlockSpec(memory_space=pl.ANY)
    vmem = pl.BlockSpec(memory_space=pltpu.VMEM)
    groups = experts // GROUP
    shape_gate = jax.ShapeDtypeStruct((experts, height * n, width // n), narrow)
    shape_down = jax.ShapeDtypeStruct((experts, inner // n, share * n), narrow)
    piece = 2 * experts * (2 * height * width + inner * share)
    raw_gate, raw_up, raw_down, router = pl.pallas_call(
        functools.partial(exchange_kernel, n, banks),
        out_shape=(
            shape_gate,
            shape_gate,
            shape_down,
            jax.ShapeDtypeStruct((rows * banks, columns * n), narrow),
        ),
        in_specs=[any_space] * 3 + [vmem] * 2,
        out_specs=[any_space] * 3 + [vmem],
        scratch_shapes=[
            pltpu.VMEM((2, GROUP, height, width), jnp.float32),
            pltpu.VMEM((2, GROUP, height, width), jnp.float32),
            pltpu.VMEM((2, GROUP, inner, share), jnp.float32),
            pltpu.VMEM((n, experts, height, width // n), narrow),
            pltpu.VMEM((n, experts, height, width // n), narrow),
            pltpu.VMEM((n, experts, inner // n, share), narrow),
            pltpu.VMEM((rows, columns), narrow),
            pltpu.VMEM((rows * banks, columns * n), narrow),
            pltpu.SemaphoreType.DMA((3, 2)),
            pltpu.SemaphoreType.DMA((3, groups)),
            pltpu.SemaphoreType.DMA((3, groups, n)),
            pltpu.SemaphoreType.DMA((3, groups, n)),
            pltpu.SemaphoreType.DMA((2, n)),
            pltpu.SemaphoreType.DMA((2, banks)),
        ],
        compiler_params=pltpu.CompilerParams(
            collective_id=0, has_side_effects=True, vmem_limit_bytes=60 * 2**20
        ),
        cost_estimate=pl.CostEstimate(flops=piece, bytes_accessed=3 * piece, transcendentals=0),
        name="exchange",
    )(master_gate, master_up, master_down, router_weight.T, router_gain[None, :])

    def block(shape):
        return pl.BlockSpec((BATCH,) + shape.shape[1:], lambda e: (e, 0, 0))

    def whole(shape):
        return pl.BlockSpec(shape.shape, lambda e: (0, 0))

    scales_gate = jax.ShapeDtypeStruct((experts, width // n), jnp.float32)
    scales_down = jax.ShapeDtypeStruct((experts, inner // n), jnp.float32)
    outs = (shape_gate, shape_gate, shape_down)
    scales = (scales_gate, scales_gate, scales_down)
    results = pl.pallas_call(
        functools.partial(scale_kernel, n),
        grid=(experts // BATCH,),
        out_shape=outs + scales,
        in_specs=[block(s) for s in outs],
        out_specs=[block(s) for s in outs] + [whole(s) for s in scales],
        compiler_params=pltpu.CompilerParams(vmem_limit_bytes=60 * 2**20),
        name="scale",
    )(raw_gate, raw_up, raw_down)
    return (*results, router.T)


def plain(master_gate, master_up, master_down, router_weight, router_gain):
    total_gate, total_up, total_down = (
        lax.psum(jnp.sum(master_gate * master_gate, axis=1).astype(jnp.bfloat16), "zero").astype(
            jnp.float32
        ),
        lax.psum(jnp.sum(master_up * master_up, axis=1).astype(jnp.bfloat16), "zero").astype(
            jnp.float32
        ),
        lax.psum(jnp.sum(master_down * master_down, axis=2).astype(jnp.bfloat16), "zero").astype(
            jnp.float32
        ),
    )
    scale_gate = jnp.sqrt(total_gate)
    scale_up = jnp.sqrt(total_up)
    scale_down = jnp.sqrt(total_down)
    narrow_gate, narrow_up, narrow_down = (
        (master_gate / jnp.expand_dims(scale_gate, 1)).astype(jnp.bfloat16),
        (master_up / jnp.expand_dims(scale_up, 1)).astype(jnp.bfloat16),
        (master_down / jnp.expand_dims(scale_down, 2)).astype(jnp.bfloat16),
    )
    final_gate, final_up = (
        lax.all_to_all(narrow_gate, "zero", split_axis=2, concat_axis=1, tiled=True),
        lax.all_to_all(narrow_up, "zero", split_axis=2, concat_axis=1, tiled=True),
    )
    final_down = lax.all_to_all(narrow_down, "zero", split_axis=1, concat_axis=2, tiled=True)
    scale_gate = lax.dynamic_slice_in_dim(
        scale_gate, lax.axis_index("zero") * final_gate.shape[2], final_gate.shape[2], axis=1
    )
    scale_up = lax.dynamic_slice_in_dim(
        scale_up, lax.axis_index("zero") * final_up.shape[2], final_up.shape[2], axis=1
    )
    scale_down = lax.dynamic_slice_in_dim(
        scale_down, lax.axis_index("zero") * final_down.shape[1], final_down.shape[1], axis=1
    )
    part_router = (router_weight * router_gain[:, None]).astype(jnp.bfloat16)
    row_router = lax.all_gather(part_router, "zero", axis=0, tiled=True)
    serve_router = lax.all_gather(row_router, "bank", axis=1, tiled=True)
    return (final_gate, final_up, final_down, scale_gate, scale_up, scale_down, serve_router)


def local(n, banks, master_gate, master_up, master_down, router_weight, router_gain):
    experts, height, width = master_gate.shape
    inner, share = master_down.shape[1:]
    columns, rows = router_weight.shape
    tiled = (
        experts % GROUP == 0
        and experts % BATCH == 0
        and height % LANES == 0
        and width // n == LANES
        and inner // n == LANES
        and share % LANES == 0
        and columns % LANES == 0
        and rows % ROWS == 0
    )
    arrays = (master_gate, master_up, master_down, router_weight, router_gain)
    return fused(n, banks, *arrays) if tiled else plain(*arrays)


def solution(mesh):
    in_specs = (
        P("bank", "zero", None),
        P("bank", "zero", None),
        P("bank", None, "zero"),
        P("zero", "bank"),
        P("zero"),
    )
    out_specs = (
        P("bank", None, "zero"),
        P("bank", None, "zero"),
        P("bank", "zero", None),
        P("bank", "zero"),
        P("bank", "zero"),
        P("bank", "zero"),
        P(),
    )
    body = functools.partial(local, mesh.shape["zero"], mesh.shape["bank"])
    return jax.shard_map(body, mesh=mesh, in_specs=in_specs, out_specs=out_specs, check_vma=False)
```
